32 devices in a mesh: row: 4 (over y, core), col: 8 (over z, x).
Axes of the slice: x: 2, y: 2, z: 4, core: 2. Of those that a mesh axis runs over, the one named last changes fastest.
Arguments:
- acts: bfloat16 [192, 2, 28672], P('col', None, 'row'), may hold values from -6 to 6
- grads: bfloat16 [192, 2, 8192], P('row', None, 'col'), may hold values from -0.3984375 to 0.3984375
- basis_in: bfloat16 [28672, 28672], P('row', 'col'), may hold values from -0.03125 to 0.03125
- basis_out: bfloat16 [8192, 8192], P('col', 'row'), may hold values from -0.0625 to 0.0625
- eigen: bfloat16 [28672, 8192], P('col', 'row'), may hold values from 0.5 to 8
- sketch: bfloat16 [72, 8192], P(None, 'col'), may hold values from -0.0625 to 0.0625
Outputs:
- range_basis: float32 [2, 72, 28672], P(None, None, 'row')
- projected: float32 [2, 72, 8192], P(None, None, 'col')
The draws below stay inside these ranges and needn't reach their ends.
All inputs are finite; a program needn't handle non-finite values.
Results may differ from the reference program's by a relative error of at most 0.018.
Values may be sent and summed in bfloat16 or wider, within the bound.
A program may use at most 192 MiB of HBM per device.

```python
import math
import jax
import jax.numpy as jnp
from jax import lax

IN = 28672
OUT = 8192
SK = 72
NQ = 2
TOK = 192


def steps_of(own_key, shape, shards, low, largest):
    loudness = 1.0
    for position, parts in shards:
        steps = jax.random.uniform(jax.random.fold_in(jax.random.fold_in(own_key, 6), position), (parts,), jnp.float32, low / len(shards), largest / len(shards))
        loudness = loudness * jnp.repeat(jnp.exp(steps), shape[position] // parts).reshape((-1,) + (1,) * (len(shape) - 1 - position))
    return loudness


def bell_draw(rng, shape, spread, bound, shards=(), dtype=jnp.bfloat16):
    level = steps_of(rng, shape, shards, -0.22, 0.18) if shards else 1.0
    values = jax.random.normal(rng, shape, jnp.float32) * spread * level
    return jnp.minimum(jnp.maximum(values, -bound), bound).astype(dtype)


def setup_inputs(seed: int = 0) -> dict:
    splits = jax.random.split(jax.random.key(seed), 7)
    return {
        "acts": bell_draw(splits[0], (TOK, NQ, IN), 1.0, 6.0, ((0, 8), (2, 4))),
        "grads": bell_draw(splits[1], (TOK, NQ, OUT), 0.0625, 0.3984375, ((0, 4), (2, 8))),
        "basis_in": bell_draw(splits[2], (IN, IN), IN ** -0.5, 0.03125, ((0, 4), (1, 8))),
        "basis_out": bell_draw(splits[3], (OUT, OUT), OUT ** -0.5, 0.0625, ((0, 8), (1, 4))),
        "eigen": jnp.clip(jnp.exp(math.log(8.0) - 2.7725887 * jax.random.uniform(splits[4], (IN, OUT), jnp.float32) ** steps_of(splits[4], (IN, OUT), ((0, 8), (1, 4)), -0.2, 0.2)), 0.5, 8.0).astype(jnp.bfloat16),
        "sketch": bell_draw(splits[5], (SK, OUT), OUT ** -0.5, 0.0625, ((1, 8),)),
    }


def reference(acts, grads, basis_in, basis_out, eigen, sketch):
    act_rot = jnp.dot(acts.reshape(TOK * NQ, IN).astype(jnp.float32), basis_in.astype(jnp.float32), preferred_element_type=jnp.float32).astype(jnp.bfloat16).reshape(TOK, NQ, IN)
    grad_rot = jnp.dot(grads.reshape(TOK * NQ, OUT).astype(jnp.float32), basis_out.astype(jnp.float32), preferred_element_type=jnp.float32).astype(jnp.bfloat16).reshape(TOK, NQ, OUT)
    sketch_rot = jnp.dot(sketch.astype(jnp.float32), basis_out.astype(jnp.float32), preferred_element_type=jnp.float32).astype(jnp.bfloat16)
    eigen_wide = eigen.astype(jnp.float32)
    bases = []
    projections = []
    for query in range(NQ):
        core_sum = jnp.dot(act_rot[:, query, :].T.astype(jnp.float32), grad_rot[:, query, :].astype(jnp.float32), preferred_element_type=jnp.float32)
        scaled = (core_sum / eigen_wide).astype(jnp.bfloat16)
        reduced = jnp.dot(sketch_rot.astype(jnp.float32), scaled.T.astype(jnp.float32), preferred_element_type=jnp.float32).astype(jnp.bfloat16)
        range_rows = jnp.dot(reduced.astype(jnp.float32), basis_in.T.astype(jnp.float32), preferred_element_type=jnp.float32)
        gram = jnp.dot(range_rows, range_rows.T, precision=lax.Precision.HIGHEST)
        factor = jnp.linalg.cholesky(gram)
        basis_rows = lax.linalg.triangular_solve(factor, range_rows, left_side=True, lower=True)
        mapped = jnp.dot(basis_rows.astype(jnp.bfloat16).astype(jnp.float32), basis_in.astype(jnp.float32), preferred_element_type=jnp.float32).astype(jnp.bfloat16)
        core = jnp.dot(mapped.astype(jnp.float32), scaled.astype(jnp.float32), preferred_element_type=jnp.float32).astype(jnp.bfloat16)
        projection = jnp.dot(core.astype(jnp.float32), basis_out.T.astype(jnp.float32), preferred_element_type=jnp.float32)
        bases.append(basis_rows)
        projections.append(projection)
    return (jnp.stack(bases), jnp.stack(projections))
```

```python
import functools
import jax
import jax.numpy as jnp
from jax import lax
from jax.experimental import pallas as pl
from jax.experimental.pallas import tpu as pltpu
from jax.sharding import PartitionSpec as P

MESH = pl.DeviceIdType.MESH
VMEM = pl.BlockSpec(memory_space=pltpu.VMEM)
BAND = 16
PIECES = 3
BF = jnp.bfloat16
F32 = jnp.float32


def remote(src, dst, send_sem, recv_sem, axis, peer):
    return pltpu.make_async_remote_copy(
        src_ref=src,
        dst_ref=dst,
        send_sem=send_sem,
        recv_sem=recv_sem,
        device_id={axis: peer},
        device_id_type=MESH,
    )


def greet(axis, n, me):
    barrier = pltpu.get_barrier_semaphore()
    for k in range(1, n):
        pl.semaphore_signal(
            barrier, inc=1, device_id={axis: lax.rem(me + k, n)}, device_id_type=MESH
        )
    pl.semaphore_wait(barrier, n - 1)


def columns(ref, index, width):
    return ref.at[:, pl.ds(pl.multiple_of(index * width, width), width)]


def line_gather(n, me, own, view, sems):
    z_send, z_recv, x_send, x_recv = sems
    nz = n // 2
    z, x = me // 2, lax.rem(me, 2)
    other = me + 1 - 2 * x

    def along(step, origin, c, src):
        block = view(origin * 2 + x, c)
        way = (step + 1) // 2
        return remote(
            src, block, z_send.at[way, origin, c], z_recv.at[origin, c], "col", me + 2 * step
        )

    def across(origin, c, src):
        block = view(origin * 2 + x, c)
        return remote(src, block, x_send.at[origin, c], x_recv.at[origin, c], "col", other)

    def arrived(origin, c):
        block = view(origin * 2 + x, c)
        remote(block, block, z_send.at[0, origin, c], z_recv.at[origin, c], "col", other).wait_recv()
        return block

    for c in range(PIECES):

        @pl.when(z < nz - 1)
        def _():
            along(1, z, c, own(c)).start()

        @pl.when(z > 0)
        def _():
            along(-1, z, c, own(c)).start()

        across(z, c, own(c)).start()

    for d in range(1, nz):
        for c in range(PIECES):

            @pl.when(z >= d)
            def _():
                block = arrived(z - d, c)

                @pl.when(z < nz - 1)
                def _():
                    along(1, z - d, c, block).start()

                across(z - d, c, block).start()

            @pl.when(z + d < nz)
            def _():
                block = arrived(z + d, c)

                @pl.when(z > 0)
                def _():
                    along(-1, z + d, c, block).start()

                across(z + d, c, block).start()

    def finish():
        for o in range(nz):
            for c in range(PIECES):
                across(o, c, view(o * 2 + x, c)).wait_send()
                block = view(o * 2 + 1 - x, c)
                remote(block, block, x_send.at[o, c], x_recv.at[o, c], "col", other).wait_recv()

                @pl.when((z < nz - 1) & (z >= o))
                def _():
                    along(1, o, c, view(o * 2 + x, c)).wait_send()

                @pl.when((z > 0) & (z <= o))
                def _():
                    along(-1, o, c, view(o * 2 + x, c)).wait_send()

    return finish


def gather_sems(n):
    nz = n // 2
    return [
        pltpu.SemaphoreType.DMA((2, nz, PIECES)),
        pltpu.SemaphoreType.DMA((nz, PIECES)),
        pltpu.SemaphoreType.DMA((nz, PIECES)),
        pltpu.SemaphoreType.DMA((nz, PIECES)),
    ]


def gather_kernel(n, x_ref, o_ref, own_sem, *sems):
    me = lax.axis_index("col")
    rows = x_ref.shape[0] // PIECES
    greet("col", n, me)
    own = pltpu.make_async_copy(x_ref, o_ref.at[me], own_sem)
    own.start()
    finish = line_gather(
        n,
        me,
        lambda c: x_ref.at[pl.ds(c * rows, rows)],
        lambda g, c: o_ref.at[g, pl.ds(c * rows, rows)],
        sems,
    )
    own.wait()
    finish()


def row_gather_kernel(n, x_ref, o_ref, send_sem, recv_sem, own_sem):
    me = lax.axis_index("row")
    greet("row", n, me)
    copies = []
    for k in range(1, n):
        peer = lax.rem(me + k, n)
        copies.append(remote(x_ref, o_ref.at[me], send_sem.at[k], recv_sem.at[k], "row", peer))
        copies[-1].start()
    own = pltpu.make_async_copy(x_ref, o_ref.at[me], own_sem)
    own.start()
    own.wait()
    for copy in copies:
        copy.wait()


def add_into(out, rows, terms):
    def step(i, carry):
        at = pl.ds(pl.multiple_of(i * BAND, BAND), BAND)
        total = terms[0](at).astype(F32)
        for term in terms[1:]:
            total = total + term(at).astype(F32)
        out(at, total)
        return carry

    lax.fori_loop(0, rows // BAND, step, 0)


def col_sum_kernel(
    n, x_ref, o_ref, x_buf, z_buf, stage, xs, xr, zs, zr, own_sem, *sems
):
    me = lax.axis_index("col")
    nz = n // 2
    z, x = me // 2, lax.rem(me, 2)
    other = me + 1 - 2 * x
    rows, width = x_ref.shape[0], x_ref.shape[1] // n
    greet("col", n, me)
    order = [lax.rem(z + k, nz) for k in (*range(1, nz), 0)]
    firsts, seconds = [], []
    for to in order:
        src = columns(x_ref, to * 2 + 1 - x, width)
        firsts.append(remote(src, x_buf.at[to], xs.at[to], xr.at[to], "col", other))
        firsts[-1].start()
    for to, first in zip(order[:-1], firsts):
        first.wait_recv()
        mine = pl.ds(pl.multiple_of((to * 2 + x) * width, width), width)

        def put(at, total):
            stage[to, at, :] = total.astype(BF)

        add_into(put, rows, [lambda at: x_ref[at, mine], lambda at: x_buf[to, at, :]])
        seconds.append(remote(stage.at[to], z_buf.at[z], zs.at[to], zr.at[z], "col", to * 2 + x))
        seconds[-1].start()
    firsts[-1].wait_recv()
    for source in order[:-1]:
        block = z_buf.at[source]
        remote(block, block, zs.at[source], zr.at[source], "col", other).wait_recv()
    mine = pl.ds(pl.multiple_of(me * width, width), width)

    def put_own(at, total):
        stage[z, at, :] = total.astype(BF)

    terms = [lambda at: x_ref[at, mine], lambda at: x_buf[z, at, :]]
    for source in order[:-1]:
        terms.append(lambda at, source=source: z_buf[source, at, :])
    add_into(put_own, rows, terms)
    part = rows // PIECES

    def view(g, c):
        return o_ref.at[
            pl.ds(c * part, part), pl.ds(pl.multiple_of(g * width, width), width)
        ]

    own = pltpu.make_async_copy(stage.at[z], columns(o_ref, me, width), own_sem)
    own.start()
    finish = line_gather(n, me, lambda c: stage.at[z, pl.ds(c * part, part)], view, sems)
    own.wait()
    finish()
    for copy in firsts:
        copy.wait_send()
    for copy in seconds:
        copy.wait_send()


def row_sum_kernel(
    n, pieces, x_ref, o_ref, k_buf, y_buf, stage, ks, kr, ys, yr, gs, gr
):
    me = lax.axis_index("row")
    ny = n // 2
    y, k = me // 2, lax.rem(me, 2)
    other = me + 1 - 2 * k
    width = x_ref.shape[1] // 2
    rows = x_ref.shape[0] // pieces
    mine = pl.ds(pl.multiple_of(k * width, width), width)
    theirs = pl.ds(pl.multiple_of((1 - k) * width, width), width)
    greet("row", n, me)
    parts = [pl.ds(c * rows, rows) for c in range(pieces)]
    swaps, sends, hands = [], {}, []
    for c, part in enumerate(parts):
        swaps.append(
            remote(x_ref.at[part, theirs], k_buf.at[part], ks.at[c], kr.at[c], "row", other)
        )
        swaps[-1].start()
    for c, part in enumerate(parts):
        swaps[c].wait_recv()

        def put(at, total, c=c):
            stage[pl.ds(pl.multiple_of(c * rows + at.start, BAND), BAND), :] = total.astype(BF)

        def shifted(at, c=c):
            return pl.ds(pl.multiple_of(c * rows + at.start, BAND), BAND)

        add_into(
            put,
            rows,
            [
                lambda at, s=shifted: x_ref[s(at), mine],
                lambda at, s=shifted: k_buf[s(at), :],
            ],
        )
        for d in range(1, ny):
            peer = lax.rem(y + d, ny) * 2 + k
            sends[c, d] = remote(
                stage.at[part], y_buf.at[d - 1, part], ys.at[d - 1, c], yr.at[d - 1, c], "row", peer
            )
            sends[c, d].start()
    for c, part in enumerate(parts):
        for d in range(1, ny):
            sends[c, d].wait_recv()

        def shifted(at, c=c):
            return pl.ds(pl.multiple_of(c * rows + at.start, BAND), BAND)

        def put(at, total, s=shifted):
            o_ref[s(at), mine] = total.astype(o_ref.dtype)

        terms = [lambda at, s=shifted: stage[s(at), :]]
        for d in range(1, ny):
            terms.append(lambda at, s=shifted, d=d: y_buf[d - 1, s(at), :])
        add_into(put, rows, terms)
        place = o_ref.at[part, mine]
        hands.append(remote(place, place, gs.at[c], gr.at[c], "row", other))
        hands[-1].start()
    for c in range(pieces):
        swaps[c].wait_send()
        for d in range(1, ny):
            sends[c, d].wait_send()
        hands[c].wait()


def launch(kernel, name, number, shape, dtype, scratch, x):
    return pl.pallas_call(
        kernel,
        name=name,
        out_shape=jax.ShapeDtypeStruct(shape, dtype),
        in_specs=[VMEM],
        out_specs=VMEM,
        scratch_shapes=scratch,
        compiler_params=pltpu.CompilerParams(
            collective_id=number, has_side_effects=True, vmem_limit_bytes=44 * 2**20
        ),
    )(x)


def fits(rows, width, n, pieces=PIECES):
    return n % 2 == 0 and rows % (BAND * pieces) == 0 and width % 128 == 0


def gather_col(x, n, number):
    if not fits(*x.shape, n):
        return lax.all_gather(x, "col", axis=0, tiled=True)
    kernel = functools.partial(gather_kernel, n)
    scratch = [pltpu.SemaphoreType.DMA, *gather_sems(n)]
    full = launch(kernel, f"gather{number}", number, (n, *x.shape), x.dtype, scratch, x)
    return full.reshape(n * x.shape[0], x.shape[1])


def gather_row(x, n, number):
    if not fits(*x.shape, n):
        return lax.all_gather(x, "row", axis=0, tiled=True)
    kernel = functools.partial(row_gather_kernel, n)
    sem = pltpu.SemaphoreType.DMA
    scratch = [sem((n,)), sem((n,)), sem]
    full = launch(kernel, f"gather{number}", number, (n, *x.shape), x.dtype, scratch, x)
    return full.reshape(n * x.shape[0], x.shape[1])


def col_sum(x, n, number):
    rows, width = x.shape[0], x.shape[1] // n
    if not fits(rows, width, n):
        return lax.psum(x.astype(F32), "col").astype(BF)
    nz = n // 2
    sem = pltpu.SemaphoreType.DMA
    buf = pltpu.VMEM((nz, rows, width), BF)
    scratch = [buf, buf, buf, *[sem((nz,))] * 4, sem, *gather_sems(n)]
    kernel = functools.partial(col_sum_kernel, n)
    return launch(kernel, f"sum{number}", number, x.shape, BF, scratch, x)


def row_sum(x, n, number):
    rows, width = x.shape[0], x.shape[1] // 2
    if not fits(rows, width, n):
        return lax.psum(x.astype(F32), "row").astype(BF)
    ny = n // 2
    sem = pltpu.SemaphoreType.DMA
    scratch = [
        pltpu.VMEM((rows, width), BF),
        pltpu.VMEM((max(ny - 1, 1), rows, width), BF),
        pltpu.VMEM((rows, width), BF),
        sem((PIECES,)),
        sem((PIECES,)),
        sem((max(ny - 1, 1), PIECES)),
        sem((max(ny - 1, 1), PIECES)),
        sem((PIECES,)),
        sem((PIECES,)),
    ]
    kernel = functools.partial(row_sum_kernel, n, PIECES)
    return launch(kernel, f"sum{number}", number, x.shape, BF, scratch, x)


def factor_kernel(n, size, g_ref, o_ref, slots, work, send_sem, recv_sem):
    me = lax.axis_index("row")
    queries, high, wide = o_ref.shape
    greet("row", n, me)
    copies = []
    for k in range(1, n):
        peer = lax.rem(me + k, n)
        copies.append(
            remote(g_ref, slots.at[me], send_sem.at[k], recv_sem.at[k], "row", peer)
        )
        copies[-1].start()
    slots[me] = g_ref[...]
    for copy in copies:
        copy.wait()
    total = slots[0]
    for k in range(1, n):
        total = total + slots[k]
    work[...] = total
    row = lax.broadcasted_iota(jnp.int32, (high, wide), 0)
    lane = lax.broadcasted_iota(jnp.int32, (high, wide), 1)

    def step(k, carry):
        for q in range(queries):
            t = work[q]
            top = work[q, pl.ds(k, 1), :]
            column = jnp.sum(jnp.where(lane == k, t, 0.0), axis=1, keepdims=True)
            pivot = jnp.sum(jnp.where(lane[:1] == k, top, 0.0), axis=1, keepdims=True)
            part = column / pivot
            top = jnp.where(lane[:1] == k, 0.0, top)
            base = jnp.where(lane == k, 0.0, t)
            moved = jnp.where(lane == k, -part, base - part * top)
            work[q] = jnp.where(row > k, moved, t)
        return carry

    lax.fori_loop(0, size, step, 0)
    for q in range(queries):
        t = work[q]
        diagonal = jnp.sum(jnp.where(lane == row, t, 0.0), axis=1, keepdims=True)
        scale = lax.rsqrt(diagonal)
        scale = scale * (1.5 - 0.5 * diagonal * scale * scale)
        o_ref[q] = jnp.where(lane < row, t * scale, jnp.where(lane == row, scale, 0.0))


def inverse_factor(gram, n, number):
    queries, size, _ = gram.shape
    if n % 2 or size > 128 or size % 8:
        factor = jnp.linalg.cholesky(lax.psum(gram, "row"))
        unit = jnp.broadcast_to(jnp.eye(size, dtype=F32), gram.shape)
        return lax.linalg.triangular_solve(factor, unit, left_side=True, lower=True)
    wide = jnp.pad(gram, ((0, 0), (0, 0), (0, 128 - size)))
    sem = pltpu.SemaphoreType.DMA
    scratch = [pltpu.VMEM((n, *wide.shape), F32), pltpu.VMEM(wide.shape, F32), sem((n,)), sem((n,))]
    kernel = functools.partial(factor_kernel, n, size)
    return launch(kernel, f"factor{number}", number, wide.shape, F32, scratch, wide)[:, :, :size]


def scale_kernel(act_ref, grad_ref, eigen_ref, sketch_ref, scaled_ref, reduced_ref):
    inverse = 1.0 / eigen_ref[...].astype(F32)
    for q in range(act_ref.shape[0]):
        total = lax.dot_general(
            act_ref[q], grad_ref[q], (((0,), (0,)), ((), ())), preferred_element_type=F32
        )
        scaled = (total * inverse).astype(BF)
        scaled_ref[q] = scaled
        part = lax.dot_general(
            sketch_ref[...], scaled, (((1,), (1,)), ((), ())), preferred_element_type=F32
        )
        reduced_ref[q] = part.astype(BF)


def scale_and_reduce(act, grad, eigen, sketch):
    queries, tokens, wide = act.shape
    deep = grad.shape[2]
    size = sketch.shape[0]
    tile = 256
    if wide % tile or deep % 128 or tokens % 8 or size % 8:
        total = jnp.einsum("qtj,qtp->qjp", act, grad, preferred_element_type=F32)
        scaled = (total / eigen.astype(F32)).astype(BF)
        part = jnp.einsum("qjp,sp->qsj", scaled, sketch, preferred_element_type=F32)
        return scaled, part.astype(BF)
    return pl.pallas_call(
        scale_kernel,
        name="scale",
        grid=(wide // tile,),
        in_specs=[
            pl.BlockSpec((queries, tokens, tile), lambda i: (0, 0, i)),
            pl.BlockSpec((queries, tokens, deep), lambda i: (0, 0, 0)),
            pl.BlockSpec((tile, deep), lambda i: (i, 0)),
            pl.BlockSpec((size, deep), lambda i: (0, 0)),
        ],
        out_specs=[
            pl.BlockSpec((queries, tile, deep), lambda i: (0, i, 0)),
            pl.BlockSpec((queries, size, tile), lambda i: (0, 0, i)),
        ],
        out_shape=[
            jax.ShapeDtypeStruct((queries, wide, deep), BF),
            jax.ShapeDtypeStruct((queries, size, wide), BF),
        ],
        compiler_params=pltpu.CompilerParams(vmem_limit_bytes=44 * 2**20),
    )(act, grad, eigen, sketch)


def dot(a, b, contract):
    return lax.dot_general(a, b, ((contract), ((), ())), preferred_element_type=F32)


def on_device(nrow, ncol, acts, grads, basis_in, basis_out, eigen, sketch):
    queries = acts.shape[1]
    size = sketch.shape[0]
    flat = queries * size
    full_grads = gather_row(grads.reshape(-1, grads.shape[2]), nrow, 0)
    rows = full_grads.shape[0]
    tokens = rows // queries
    joined = jnp.concatenate([full_grads, sketch], axis=0)
    joined = jnp.pad(joined, ((0, -joined.shape[0] % (BAND * PIECES)), (0, 0)))
    joined_sum = col_sum(dot(joined, basis_out, ((1,), (0,))).astype(BF), ncol, 1)
    grad_rot = joined_sum[:rows].reshape(tokens, queries, -1).transpose(1, 0, 2)
    sketch_rot = joined_sum[rows : rows + size]
    full_acts = gather_col(acts.reshape(-1, acts.shape[2]), ncol, 2)
    act_rot = row_sum(dot(full_acts, basis_in, ((1,), (0,))).astype(BF), nrow, 3)
    act_rot = act_rot.reshape(tokens, queries, -1).transpose(1, 0, 2)
    scaled, reduced_part = scale_and_reduce(act_rot, grad_rot, eigen, sketch_rot)
    reduced = row_sum(reduced_part.reshape(flat, -1), nrow, 4)
    range_part = dot(reduced, basis_in, ((1,), (1,))).astype(BF)
    range_rows = col_sum(range_part, ncol, 5).reshape(queries, size, -1)
    gram = jnp.einsum("qsi,qri->qsr", range_rows, range_rows, preferred_element_type=F32)
    inverse = inverse_factor(gram, nrow, 6)
    range_basis = jnp.einsum(
        "qsr,qri->qsi", inverse, range_rows.astype(F32), precision=lax.Precision.HIGHEST
    )
    basis_rows = range_basis.astype(BF).reshape(flat, -1)
    mapped = row_sum(dot(basis_rows, basis_in, ((1,), (0,))).astype(BF), nrow, 7)
    mapped = mapped.reshape(queries, size, -1)
    core_part = jnp.einsum("qsj,qjp->qsp", mapped, scaled, preferred_element_type=F32)
    core = col_sum(core_part.astype(BF).reshape(flat, -1), ncol, 8)
    projection_part = dot(core, basis_out, ((1,), (1,))).astype(BF)
    projected = row_sum(projection_part, nrow, 9)
    return range_basis, projected.astype(F32).reshape(queries, size, -1)


def solution(mesh):
    in_specs = (
        P("col", None, "row"),
        P("row", None, "col"),
        P("row", "col"),
        P("col", "row"),
        P("col", "row"),
        P(None, "col"),
    )
    out_specs = (P(None, None, "row"), P(None, None, "col"))
    body = functools.partial(on_device, mesh.shape["row"], mesh.shape["col"])
    return jax.shard_map(body, mesh=mesh, in_specs=in_specs, out_specs=out_specs, check_vma=False)
```

```python
import functools
import jax
import jax.numpy as jnp
from jax import lax
from jax.experimental import pallas as pl
from jax.experimental.pallas import tpu as pltpu
from jax.sharding import PartitionSpec as P

MESH = pl.DeviceIdType.MESH
VMEM = pl.BlockSpec(memory_space=pltpu.VMEM)
BAND = 16
PIECES = 3
TILE = 256
DEPTH = 3
LAG = 4
GAP = 3
ANY = pl.BlockSpec(memory_space=pl.ANY)
BF = jnp.bfloat16
F32 = jnp.float32


def remote(src, dst, send_sem, recv_sem, axis, peer):
    return pltpu.make_async_remote_copy(
        src_ref=src,
        dst_ref=dst,
        send_sem=send_sem,
        recv_sem=recv_sem,
        device_id={axis: peer},
        device_id_type=MESH,
    )


def greet(axis, n, me):
    barrier = pltpu.get_barrier_semaphore()
    for k in range(1, n):
        pl.semaphore_signal(
            barrier, inc=1, device_id={axis: lax.rem(me + k, n)}, device_id_type=MESH
        )
    pl.semaphore_wait(barrier, n - 1)


def columns(ref, index, width):
    return ref.at[:, pl.ds(pl.multiple_of(index * width, width), width)]


def line_gather(n, me, own, view, sems):
    z_send, z_recv, x_send, x_recv = sems
    nz = n // 2
    z, x = me // 2, lax.rem(me, 2)
    other = me + 1 - 2 * x

    def along(step, origin, c, src):
        block = view(origin * 2 + x, c)
        way = (step + 1) // 2
        return remote(
            src, block, z_send.at[way, origin, c], z_recv.at[origin, c], "col", me + 2 * step
        )

    def across(origin, c, src):
        block = view(origin * 2 + x, c)
        return remote(src, block, x_send.at[origin, c], x_recv.at[origin, c], "col", other)

    def arrived(origin, c):
        block = view(origin * 2 + x, c)
        remote(block, block, z_send.at[0, origin, c], z_recv.at[origin, c], "col", other).wait_recv()
        return block

    for c in range(PIECES):

        @pl.when(z < nz - 1)
        def _():
            along(1, z, c, own(c)).start()

        @pl.when(z > 0)
        def _():
            along(-1, z, c, own(c)).start()

        across(z, c, own(c)).start()

    def relay():
        for d in range(1, nz):
            for c in range(PIECES):

                @pl.when(z >= d)
                def _():
                    block = arrived(z - d, c)

                    @pl.when(z < nz - 1)
                    def _():
                        along(1, z - d, c, block).start()

                    across(z - d, c, block).start()

                @pl.when(z + d < nz)
                def _():
                    block = arrived(z + d, c)

                    @pl.when(z > 0)
                    def _():
                        along(-1, z + d, c, block).start()

                    across(z + d, c, block).start()

    def finish():
        for o in range(nz):
            for c in range(PIECES):
                across(o, c, view(o * 2 + x, c)).wait_send()
                block = view(o * 2 + 1 - x, c)
                remote(block, block, x_send.at[o, c], x_recv.at[o, c], "col", other).wait_recv()

                @pl.when((z < nz - 1) & (z >= o))
                def _():
                    along(1, o, c, view(o * 2 + x, c)).wait_send()

                @pl.when((z > 0) & (z <= o))
                def _():
                    along(-1, o, c, view(o * 2 + x, c)).wait_send()

    return relay, finish


def gather_sems(n):
    nz = n // 2
    return [
        pltpu.SemaphoreType.DMA((2, nz, PIECES)),
        pltpu.SemaphoreType.DMA((nz, PIECES)),
        pltpu.SemaphoreType.DMA((nz, PIECES)),
        pltpu.SemaphoreType.DMA((nz, PIECES)),
    ]


def gather_both_kernel(
    ncol, nrow, x_ref, g_ref, o_ref, p_ref, own_sem, send_sem, recv_sem, own_two, *sems
):
    me, mine = lax.axis_index("col"), lax.axis_index("row")
    rows = x_ref.shape[0] // PIECES
    greet_both(ncol, nrow, me, mine)
    relay, finish = line_gather(
        ncol,
        me,
        lambda c: x_ref.at[pl.ds(c * rows, rows)],
        lambda g, c: o_ref.at[g, pl.ds(c * rows, rows)],
        sems,
    )
    copies = []
    for k in range(1, nrow):
        peer = lax.rem(mine + k, nrow)
        copies.append(remote(g_ref, p_ref.at[mine], send_sem.at[k], recv_sem.at[k], "row", peer))
        copies[-1].start()
    own = pltpu.make_async_copy(x_ref, o_ref.at[me], own_sem)
    own.start()
    two = pltpu.make_async_copy(g_ref, p_ref.at[mine], own_two)
    two.start()
    own.wait()
    two.wait()
    relay()
    finish()
    for copy in copies:
        copy.wait()


def greet_both(ncol, nrow, me, mine):
    barrier = pltpu.get_barrier_semaphore()
    for k in range(1, ncol):
        pl.semaphore_signal(
            barrier, inc=1, device_id={"col": lax.rem(me + k, ncol)}, device_id_type=MESH
        )
    for k in range(1, nrow):
        pl.semaphore_signal(
            barrier, inc=1, device_id={"row": lax.rem(mine + k, nrow)}, device_id_type=MESH
        )
    pl.semaphore_wait(barrier, ncol + nrow - 2)


def add_into(out, rows, terms):
    def step(i, carry):
        at = pl.ds(pl.multiple_of(i * BAND, BAND), BAND)
        total = terms[0](at).astype(F32)
        for term in terms[1:]:
            total = total + term(at).astype(F32)
        out(at, total)
        return carry

    lax.fori_loop(0, rows // BAND, step, 0)


def col_sum_stages(
    n, me, x_ref, o_ref, x_buf, z_buf, stage, xs, xr, zs, zr, own_sem, *sems
):
    nz = n // 2
    z, x = me // 2, lax.rem(me, 2)
    other = me + 1 - 2 * x
    rows, width = x_ref.shape[0], x_ref.shape[1] // n
    part = rows // PIECES
    order = [lax.rem(z + k, nz) for k in (*range(1, nz), 0)]

    def first(to):
        src = columns(x_ref, to * 2 + 1 - x, width)
        return remote(src, x_buf.at[to], xs.at[to], xr.at[to], "col", other)

    def second(to):
        return remote(stage.at[to], z_buf.at[z], zs.at[to], zr.at[z], "col", to * 2 + x)

    def begin():
        for to in order:
            first(to).start()

    def pair(to):
        first(to).wait_recv()
        mine = pl.ds(pl.multiple_of((to * 2 + x) * width, width), width)

        def put(at, total):
            stage[to, at, :] = total.astype(BF)

        add_into(put, rows, [lambda at: x_ref[at, mine], lambda at: x_buf[to, at, :]])
        second(to).start()

    def view(g, c):
        return o_ref.at[
            pl.ds(c * part, part), pl.ds(pl.multiple_of(g * width, width), width)
        ]

    def gather():
        return line_gather(n, me, lambda c: stage.at[z, pl.ds(c * part, part)], view, sems)

    def total():
        first(z).wait_recv()
        for source in order[:-1]:
            block = z_buf.at[source]
            remote(block, block, zs.at[source], zr.at[source], "col", other).wait_recv()
        mine = pl.ds(pl.multiple_of(me * width, width), width)

        def put(at, value):
            stage[z, at, :] = value.astype(BF)

        terms = [lambda at: x_ref[at, mine], lambda at: x_buf[z, at, :]]
        for source in order[:-1]:
            terms.append(lambda at, source=source: z_buf[source, at, :])
        add_into(put, rows, terms)
        own = pltpu.make_async_copy(stage.at[z], columns(o_ref, me, width), own_sem)
        own.start()
        relay, finish = gather()
        own.wait()
        relay()
        finish()
        for to in order:
            first(to).wait_send()
        for to in order[:-1]:
            second(to).wait_send()

    return [begin, *[functools.partial(pair, to) for to in order[:-1]], total]


def col_sum_kernel(n, *refs):
    me = lax.axis_index("col")
    greet("col", n, me)
    for stage in col_sum_stages(n, me, *refs):
        stage()


def col_sum_scratch(n, rows, width):
    nz = n // 2
    sem = pltpu.SemaphoreType.DMA
    buf = pltpu.VMEM((nz, rows, width), BF)
    return [buf, buf, buf, *[sem((nz,))] * 4, sem, *gather_sems(n)]


def tile_sum(me, count, tile, part, o_ref, k_buf, y_buf, stage, ks, kr, ys, yr, gs, gr):
    y, k = me // 2, lax.rem(me, 2)
    other = me + 1 - 2 * k
    across = (1 - y) * 2 + k
    half = tile // 2
    mine = pl.ds(pl.multiple_of(k * half, half), half)
    theirs = pl.ds(pl.multiple_of((1 - k) * half, half), half)

    def spot(i):
        return pl.ds(pl.multiple_of(i * tile + k * half, half), half)

    def swap(i):
        return remote(part.at[i, :, theirs], k_buf.at[i], ks.at[i], kr.at[i], "row", other)

    def cross(i):
        return remote(stage.at[i], y_buf.at[i], ys.at[i], yr.at[i], "row", across)

    def hand(i):
        place = o_ref.at[:, spot(i)]
        return remote(place, place, gs.at[i], gr.at[i], "row", other)

    def middle(i):
        swap(i).wait_recv()
        stage[i] = (part[i, :, mine].astype(F32) + k_buf[i].astype(F32)).astype(BF)
        cross(i).start()

    def last(i):
        cross(i).wait_recv()
        o_ref[:, spot(i)] = (stage[i].astype(F32) + y_buf[i].astype(F32)).astype(BF)
        hand(i).start()

    def finish():
        def step(i, carry):
            swap(i).wait_send()
            cross(i).wait_send()
            hand(i).wait()
            return carry

        lax.fori_loop(0, count, step, 0)

    return swap, middle, last, finish


def tile_scratch(count, rows, tile):
    sem = pltpu.SemaphoreType.DMA
    half = pltpu.VMEM((count, rows, tile // 2), BF)
    return [pltpu.VMEM((count, rows, tile), BF), half, half, half, *[sem((count,))] * 6]


def tile_loop(count, compute, swap, middle, last, hooks):
    def step(i, carry):
        @pl.when(i < count)
        def _():
            compute(i)
            swap(i).start()

        @pl.when((i >= 1) & (i <= count))
        def _():
            middle(i - 1)

        @pl.when(i >= LAG)
        def _():
            last(i - LAG)

        for at, hook in hooks:
            pl.when(i == at)(hook)
        return carry

    lax.fori_loop(0, count + LAG, step, 0)


def stream_parts(n, me, a_ref, w_ref, o_ref, w_buf, w_sem, part, *rest):
    tile = w_buf.shape[2]
    count = w_ref.shape[1] // tile

    def fetch(i):
        at = pl.ds(pl.multiple_of(i * tile, tile), tile)
        slot = lax.rem(i, DEPTH)
        return pltpu.make_async_copy(w_ref.at[:, at], w_buf.at[slot], w_sem.at[slot])

    def compute(i):
        fetch(i).wait()

        @pl.when(i + DEPTH - 1 < count)
        def _():
            fetch(i + DEPTH - 1).start()

        product = jnp.dot(a_ref[...], w_buf[lax.rem(i, DEPTH)], preferred_element_type=F32)
        part[i] = product.astype(BF)

    for i in range(min(DEPTH - 1, count)):
        fetch(i).start()
    return count, compute, tile_sum(me, count, tile, part, o_ref, *rest)


def stream_scratch(count, rows, deep, tile):
    return [
        pltpu.VMEM((DEPTH, deep, tile), BF),
        pltpu.SemaphoreType.DMA((DEPTH,)),
        *tile_scratch(count, rows, tile),
    ]


def stream_kernel(n, a_ref, w_ref, o_ref, *scratch):
    me = lax.axis_index("row")
    count, compute, (swap, middle, last, finish) = stream_parts(
        n, me, a_ref, w_ref, o_ref, *scratch
    )
    greet("row", n, me)
    tile_loop(count, compute, swap, middle, last, [])
    finish()


STREAM = 12


def stream_both_kernel(n, ncol, a_ref, w_ref, x_ref, o_ref, s_ref, *scratch):
    me, mine = lax.axis_index("row"), lax.axis_index("col")
    count, compute, (swap, middle, last, finish) = stream_parts(
        n, me, a_ref, w_ref, o_ref, *scratch[:STREAM]
    )
    greet_both(ncol, n, mine, me)
    begin, *pairs, total = col_sum_stages(ncol, mine, x_ref, s_ref, *scratch[STREAM:])
    begin()
    hooks = [(GAP * (k + 1), pair) for k, pair in enumerate(pairs)]
    late = [pair for at, pair in hooks if at >= count + LAG]
    hooks = [hook for hook in hooks if hook[0] < count + LAG]
    tile_loop(count, compute, swap, middle, last, hooks)
    for pair in late:
        pair()
    total()
    finish()


def row_sum_kernel(
    n, pieces, x_ref, o_ref, k_buf, y_buf, stage, ks, kr, ys, yr, gs, gr
):
    me = lax.axis_index("row")
    ny = n // 2
    y, k = me // 2, lax.rem(me, 2)
    other = me + 1 - 2 * k
    width = x_ref.shape[1] // 2
    rows = x_ref.shape[0] // pieces
    mine = pl.ds(pl.multiple_of(k * width, width), width)
    theirs = pl.ds(pl.multiple_of((1 - k) * width, width), width)
    greet("row", n, me)
    parts = [pl.ds(c * rows, rows) for c in range(pieces)]
    swaps, sends, hands = [], {}, []
    for c, part in enumerate(parts):
        swaps.append(
            remote(x_ref.at[part, theirs], k_buf.at[part], ks.at[c], kr.at[c], "row", other)
        )
        swaps[-1].start()
    for c, part in enumerate(parts):
        swaps[c].wait_recv()

        def put(at, total, c=c):
            stage[pl.ds(pl.multiple_of(c * rows + at.start, BAND), BAND), :] = total.astype(BF)

        def shifted(at, c=c):
            return pl.ds(pl.multiple_of(c * rows + at.start, BAND), BAND)

        add_into(
            put,
            rows,
            [
                lambda at, s=shifted: x_ref[s(at), mine],
                lambda at, s=shifted: k_buf[s(at), :],
            ],
        )
        for d in range(1, ny):
            peer = lax.rem(y + d, ny) * 2 + k
            sends[c, d] = remote(
                stage.at[part], y_buf.at[d - 1, part], ys.at[d - 1, c], yr.at[d - 1, c], "row", peer
            )
            sends[c, d].start()
    for c, part in enumerate(parts):
        for d in range(1, ny):
            sends[c, d].wait_recv()

        def shifted(at, c=c):
            return pl.ds(pl.multiple_of(c * rows + at.start, BAND), BAND)

        def put(at, total, s=shifted):
            o_ref[s(at), mine] = total.astype(o_ref.dtype)

        terms = [lambda at, s=shifted: stage[s(at), :]]
        for d in range(1, ny):
            terms.append(lambda at, s=shifted, d=d: y_buf[d - 1, s(at), :])
        add_into(put, rows, terms)
        place = o_ref.at[part, mine]
        hands.append(remote(place, place, gs.at[c], gr.at[c], "row", other))
        hands[-1].start()
    for c in range(pieces):
        swaps[c].wait_send()
        for d in range(1, ny):
            sends[c, d].wait_send()
        hands[c].wait()


def launch(kernel, name, number, shape, dtype, scratch, *args, specs=None, outs=None, more=None):
    out = jax.ShapeDtypeStruct(shape, dtype)
    return pl.pallas_call(
        kernel,
        name=name,
        out_shape=out if more is None else [out, more],
        in_specs=specs or [VMEM] * len(args),
        out_specs=outs or (VMEM if more is None else [VMEM, VMEM]),
        scratch_shapes=scratch,
        compiler_params=pltpu.CompilerParams(
            collective_id=number, has_side_effects=True, vmem_limit_bytes=48 * 2**20
        ),
    )(*args)


def fits(rows, width, n, pieces=PIECES):
    return n % 2 == 0 and rows % (BAND * pieces) == 0 and width % 128 == 0


def gather_both(acts, grads, nrow, ncol, number):
    if not (fits(*acts.shape, ncol) and fits(*grads.shape, nrow)):
        full = lax.all_gather(acts, "col", axis=0, tiled=True)
        return full, lax.all_gather(grads, "row", axis=0, tiled=True)
    sem = pltpu.SemaphoreType.DMA
    scratch = [sem, sem((nrow,)), sem((nrow,)), sem, *gather_sems(ncol)]
    full, part = launch(
        functools.partial(gather_both_kernel, ncol, nrow),
        f"gather{number}",
        number,
        (ncol, *acts.shape),
        BF,
        scratch,
        acts,
        grads,
        more=jax.ShapeDtypeStruct((nrow, *grads.shape), BF),
    )
    return full.reshape(-1, acts.shape[1]), part.reshape(-1, grads.shape[1])


def streams(a, w, n):
    return n == 4 and a.shape[0] % BAND == 0 and a.shape[1] % 128 == 0 and w.shape[1] % TILE == 0


def dot_row_sum(a, w, n, number):
    if not streams(a, w, n):
        return row_sum(dot(a, w, ((1,), (0,))).astype(BF), n, number)
    rows, wide = a.shape[0], w.shape[1]
    scratch = stream_scratch(wide // TILE, rows, a.shape[1], TILE)
    kernel = functools.partial(stream_kernel, n)
    return launch(
        kernel, f"stream{number}", number, (rows, wide), BF, scratch, a, w, specs=[VMEM, ANY]
    )


def dot_both_sums(a, w, x, nrow, ncol, number):
    if not (streams(a, w, nrow) and fits(x.shape[0], x.shape[1] // ncol, ncol)):
        act = row_sum(dot(a, w, ((1,), (0,))).astype(BF), nrow, number)
        return act, col_sum(x, ncol, number + 20)
    rows, wide = a.shape[0], w.shape[1]
    scratch = [
        *stream_scratch(wide // TILE, rows, a.shape[1], TILE),
        *col_sum_scratch(ncol, x.shape[0], x.shape[1] // ncol),
    ]
    return launch(
        functools.partial(stream_both_kernel, nrow, ncol),
        f"stream{number}",
        number,
        (rows, wide),
        BF,
        scratch,
        a,
        w,
        x,
        specs=[VMEM, ANY, VMEM],
        more=jax.ShapeDtypeStruct(x.shape, BF),
    )


def col_sum(x, n, number):
    rows, width = x.shape[0], x.shape[1] // n
    if not fits(rows, width, n):
        return lax.psum(x.astype(F32), "col").astype(BF)
    scratch = col_sum_scratch(n, rows, width)
    kernel = functools.partial(col_sum_kernel, n)
    return launch(kernel, f"sum{number}", number, x.shape, BF, scratch, x)


def row_sum(x, n, number):
    rows, width = x.shape[0], x.shape[1] // 2
    if not fits(rows, width, n):
        return lax.psum(x.astype(F32), "row").astype(BF)
    ny = n // 2
    sem = pltpu.SemaphoreType.DMA
    scratch = [
        pltpu.VMEM((rows, width), BF),
        pltpu.VMEM((max(ny - 1, 1), rows, width), BF),
        pltpu.VMEM((rows, width), BF),
        sem((PIECES,)),
        sem((PIECES,)),
        sem((max(ny - 1, 1), PIECES)),
        sem((max(ny - 1, 1), PIECES)),
        sem((PIECES,)),
        sem((PIECES,)),
    ]
    kernel = functools.partial(row_sum_kernel, n, PIECES)
    return launch(kernel, f"sum{number}", number, x.shape, BF, scratch, x)


def factor_kernel(n, size, g_ref, o_ref, slots, work, send_sem, recv_sem):
    me = lax.axis_index("row")
    queries, high, wide = o_ref.shape
    greet("row", n, me)
    copies = []
    for k in range(1, n):
        peer = lax.rem(me + k, n)
        copies.append(
            remote(g_ref, slots.at[me], send_sem.at[k], recv_sem.at[k], "row", peer)
        )
        copies[-1].start()
    slots[me] = g_ref[...]
    for copy in copies:
        copy.wait()
    total = slots[0]
    for k in range(1, n):
        total = total + slots[k]
    work[...] = total
    row = lax.broadcasted_iota(jnp.int32, (high, wide), 0)
    lane = lax.broadcasted_iota(jnp.int32, (high, wide), 1)

    def step(k, carry):
        for q in range(queries):
            t = work[q]
            top = work[q, pl.ds(k, 1), :]
            column = jnp.sum(jnp.where(lane == k, t, 0.0), axis=1, keepdims=True)
            pivot = jnp.sum(jnp.where(lane[:1] == k, top, 0.0), axis=1, keepdims=True)
            part = column / pivot
            top = jnp.where(lane[:1] == k, 0.0, top)
            base = jnp.where(lane == k, 0.0, t)
            moved = jnp.where(lane == k, -part, base - part * top)
            work[q] = jnp.where(row > k, moved, t)
        return carry

    lax.fori_loop(0, size, step, 0)
    for q in range(queries):
        t = work[q]
        diagonal = jnp.sum(jnp.where(lane == row, t, 0.0), axis=1, keepdims=True)
        scale = lax.rsqrt(diagonal)
        scale = scale * (1.5 - 0.5 * diagonal * scale * scale)
        o_ref[q] = jnp.where(lane < row, t * scale, jnp.where(lane == row, scale, 0.0))


def inverse_factor(gram, n, number):
    queries, size, _ = gram.shape
    if n % 2 or size > 128 or size % 8:
        factor = jnp.linalg.cholesky(lax.psum(gram, "row"))
        unit = jnp.broadcast_to(jnp.eye(size, dtype=F32), gram.shape)
        return lax.linalg.triangular_solve(factor, unit, left_side=True, lower=True)
    wide = jnp.pad(gram, ((0, 0), (0, 0), (0, 128 - size)))
    sem = pltpu.SemaphoreType.DMA
    scratch = [pltpu.VMEM((n, *wide.shape), F32), pltpu.VMEM(wide.shape, F32), sem((n,)), sem((n,))]
    kernel = functools.partial(factor_kernel, n, size)
    return launch(kernel, f"factor{number}", number, wide.shape, F32, scratch, wide)[:, :, :size]


def query_rows(value, q, queries, blocks):
    rows, wide = value.shape
    split = value.astype(F32).reshape(blocks, queries, rows // (blocks * queries), wide)
    return split[:, q].reshape(rows // queries, wide).astype(BF)


def scale_kernel(
    n, blocks, queries, act_ref, grad_ref, sketch_ref, eigen_ref, scaled_ref, o_ref,
    grad_buf, e_buf, s_buf, e_sem, s_sem, part, *rest,
):
    me = lax.axis_index("row")
    tile = e_buf.shape[1]
    count = eigen_ref.shape[0] // tile
    size = sketch_ref.shape[0]
    swap, middle, last, finish = tile_sum(me, count, tile, part, o_ref, *rest)

    def fetch(i):
        at = pl.ds(pl.multiple_of(i * tile, tile), tile)
        slot = lax.rem(i, DEPTH)
        return pltpu.make_async_copy(eigen_ref.at[at], e_buf.at[slot], e_sem.at[slot])

    def store(i):
        at = pl.ds(pl.multiple_of(i * tile, tile), tile)
        slot = lax.rem(i, 2)
        return pltpu.make_async_copy(s_buf.at[slot], scaled_ref.at[:, at], s_sem.at[slot])

    for i in range(min(DEPTH - 1, count)):
        fetch(i).start()
    for q in range(queries):
        for c in range(grad_ref.shape[1] // tile):
            at = pl.ds(c * tile, tile)
            grad_buf[q, :, at] = query_rows(grad_ref[:, at], q, queries, blocks[1])
    greet("row", n, me)

    def compute(i):
        fetch(i).wait()

        @pl.when(i + DEPTH - 1 < count)
        def _():
            fetch(i + DEPTH - 1).start()

        @pl.when(i >= 2)
        def _():
            store(i - 2).wait()

        slot = lax.rem(i, 2)
        inverse = 1.0 / e_buf[lax.rem(i, DEPTH)].astype(F32)
        act = act_ref[:, pl.ds(pl.multiple_of(i * tile, tile), tile)]
        pieces = []
        for q in range(queries):
            total = lax.dot_general(
                query_rows(act, q, queries, blocks[0]),
                grad_buf[q],
                (((0,), (0,)), ((), ())),
                preferred_element_type=F32,
            )
            scaled = (total * inverse).astype(BF)
            s_buf[slot, q] = scaled
            pieces.append(
                lax.dot_general(
                    sketch_ref[...], scaled, (((1,), (1,)), ((), ())), preferred_element_type=F32
                )
            )
        part[i] = jnp.concatenate(pieces, axis=0).astype(BF)
        store(i).start()

    tile_loop(count, compute, swap, middle, last, [])
    finish()
    for i in range(max(count - 2, 0), count):
        store(i).wait()


def scale_and_reduce(act, grad, eigen, sketch, queries, blocks, n, number):
    rows, wide = act.shape
    deep = grad.shape[1]
    size = sketch.shape[0]
    ok = n == 4 and wide % TILE == 0 and deep % TILE == 0 and size % 8 == 0
    ok = ok and queries * size % BAND == 0 and rows // queries % BAND == 0
    if not (ok and all(rows % (8 * queries * b) == 0 for b in blocks)):
        act = act.reshape(blocks[0], queries, -1, wide)
        grad = grad.reshape(blocks[1], queries, -1, deep)
        act = act.transpose(1, 0, 2, 3).reshape(queries, -1, wide)
        grad = grad.transpose(1, 0, 2, 3).reshape(queries, -1, deep)
        total = jnp.einsum("qtj,qtp->qjp", act, grad, preferred_element_type=F32)
        scaled = (total / eigen.astype(F32)).astype(BF)
        part = jnp.einsum("qjp,sp->qsj", scaled, sketch, preferred_element_type=F32)
        return scaled, row_sum(part.astype(BF).reshape(queries * size, wide), n, number)
    sem = pltpu.SemaphoreType.DMA
    scratch = [
        pltpu.VMEM((queries, rows // queries, deep), BF),
        pltpu.VMEM((DEPTH, TILE, deep), BF),
        pltpu.VMEM((2, queries, TILE, deep), BF),
        sem((DEPTH,)),
        sem((2,)),
        *tile_scratch(wide // TILE, queries * size, TILE),
    ]
    return launch(
        functools.partial(scale_kernel, n, blocks, queries),
        f"scale{number}",
        number,
        (queries, wide, deep),
        BF,
        scratch,
        act,
        grad,
        sketch,
        eigen,
        specs=[VMEM, VMEM, VMEM, ANY],
        outs=[ANY, VMEM],
        more=jax.ShapeDtypeStruct((queries * size, wide), BF),
    )


def dot(a, b, contract):
    return lax.dot_general(a, b, ((contract), ((), ())), preferred_element_type=F32)


def on_device(nrow, ncol, acts, grads, basis_in, basis_out, eigen, sketch):
    queries = acts.shape[1]
    size = sketch.shape[0]
    flat = queries * size
    full_acts, full_grads = gather_both(
        acts.transpose(1, 0, 2).reshape(-1, acts.shape[2]),
        grads.transpose(1, 0, 2).reshape(-1, grads.shape[2]),
        nrow,
        ncol,
        0,
    )
    rows = full_grads.shape[0]
    joined = jnp.concatenate([full_grads, sketch], axis=0)
    joined = jnp.pad(joined, ((0, -joined.shape[0] % (BAND * PIECES)), (0, 0)))
    joined_part = dot(joined, basis_out, ((1,), (0,))).astype(BF)
    act_rot, joined_sum = dot_both_sums(full_acts, basis_in, joined_part, nrow, ncol, 1)
    grad_rot, sketch_rot = joined_sum[:rows], joined_sum[rows : rows + size]
    scaled, reduced = scale_and_reduce(
        act_rot, grad_rot, eigen, sketch_rot, queries, (ncol, nrow), nrow, 2
    )
    range_part = dot(reduced, basis_in, ((1,), (1,))).astype(BF)
    range_rows = col_sum(range_part, ncol, 5).reshape(queries, size, -1)
    gram = jnp.einsum("qsi,qri->qsr", range_rows, range_rows, preferred_element_type=F32)
    inverse = inverse_factor(gram, nrow, 6)
    range_basis = jnp.einsum(
        "qsr,qri->qsi", inverse, range_rows.astype(F32), precision=lax.Precision.HIGHEST
    )
    basis_rows = range_basis.astype(BF).reshape(flat, -1)
    mapped = dot_row_sum(basis_rows, basis_in, nrow, 7)
    mapped = mapped.reshape(queries, size, -1)
    core_part = jnp.einsum("qsj,qjp->qsp", mapped, scaled, preferred_element_type=F32)
    core = col_sum(core_part.astype(BF).reshape(flat, -1), ncol, 8)
    projection_part = dot(core, basis_out, ((1,), (1,))).astype(BF)
    projected = row_sum(projection_part, nrow, 9)
    return range_basis, projected.astype(F32).reshape(queries, size, -1)


def solution(mesh):
    in_specs = (
        P("col", None, "row"),
        P("row", None, "col"),
        P("row", "col"),
        P("col", "row"),
        P("col", "row"),
        P(None, "col"),
    )
    out_specs = (P(None, None, "row"), P(None, None, "col"))
    body = functools.partial(on_device, mesh.shape["row"], mesh.shape["col"])
    return jax.shard_map(body, mesh=mesh, in_specs=in_specs, out_specs=out_specs, check_vma=False)
```

```python
import functools
import jax
import jax.numpy as jnp
from jax import lax
from jax.experimental import pallas as pl
from jax.experimental.pallas import tpu as pltpu
from jax.sharding import PartitionSpec as P

MESH = pl.DeviceIdType.MESH
VMEM = pl.BlockSpec(memory_space=pltpu.VMEM)
BAND = 16
PIECES = 3
TILE = 256
DEPTH = 3
LAG = 4
GAP = 3
ANY = pl.BlockSpec(memory_space=pl.ANY)
BF = jnp.bfloat16
F32 = jnp.float32


def remote(src, dst, send_sem, recv_sem, axis, peer):
    return pltpu.make_async_remote_copy(
        src_ref=src,
        dst_ref=dst,
        send_sem=send_sem,
        recv_sem=recv_sem,
        device_id={axis: peer},
        device_id_type=MESH,
    )


def greet(axis, n, me):
    barrier = pltpu.get_barrier_semaphore()
    for k in range(1, n):
        pl.semaphore_signal(
            barrier, inc=1, device_id={axis: lax.rem(me + k, n)}, device_id_type=MESH
        )
    pl.semaphore_wait(barrier, n - 1)


def columns(ref, index, width):
    return ref.at[:, pl.ds(pl.multiple_of(index * width, width), width)]


def line_gather(n, me, own, view, sems):
    z_send, z_recv, x_send, x_recv = sems
    nz = n // 2
    z, x = me // 2, lax.rem(me, 2)
    other = me + 1 - 2 * x

    def along(step, origin, c, src):
        block = view(origin * 2 + x, c)
        way = (step + 1) // 2
        return remote(
            src, block, z_send.at[way, origin, c], z_recv.at[origin, c], "col", me + 2 * step
        )

    def across(origin, c, src):
        block = view(origin * 2 + x, c)
        return remote(src, block, x_send.at[origin, c], x_recv.at[origin, c], "col", other)

    def arrived(origin, c):
        block = view(origin * 2 + x, c)
        remote(block, block, z_send.at[0, origin, c], z_recv.at[origin, c], "col", other).wait_recv()
        return block

    for c in range(PIECES):

        @pl.when(z < nz - 1)
        def _():
            along(1, z, c, own(c)).start()

        @pl.when(z > 0)
        def _():
            along(-1, z, c, own(c)).start()

        across(z, c, own(c)).start()

    def relay():
        for d in range(1, nz):
            for c in range(PIECES):

                @pl.when(z >= d)
                def _():
                    block = arrived(z - d, c)

                    @pl.when(z < nz - 1)
                    def _():
                        along(1, z - d, c, block).start()

                    across(z - d, c, block).start()

                @pl.when(z + d < nz)
                def _():
                    block = arrived(z + d, c)

                    @pl.when(z > 0)
                    def _():
                        along(-1, z + d, c, block).start()

                    across(z + d, c, block).start()

    def finish():
        for o in range(nz):
            for c in range(PIECES):
                across(o, c, view(o * 2 + x, c)).wait_send()
                block = view(o * 2 + 1 - x, c)
                remote(block, block, x_send.at[o, c], x_recv.at[o, c], "col", other).wait_recv()

                @pl.when((z < nz - 1) & (z >= o))
                def _():
                    along(1, o, c, view(o * 2 + x, c)).wait_send()

                @pl.when((z > 0) & (z <= o))
                def _():
                    along(-1, o, c, view(o * 2 + x, c)).wait_send()

    return relay, finish


def gather_sems(n):
    nz = n // 2
    return [
        pltpu.SemaphoreType.DMA((2, nz, PIECES)),
        pltpu.SemaphoreType.DMA((nz, PIECES)),
        pltpu.SemaphoreType.DMA((nz, PIECES)),
        pltpu.SemaphoreType.DMA((nz, PIECES)),
    ]


def gather_both_kernel(
    ncol, nrow, x_ref, g_ref, o_ref, p_ref, own_sem, send_sem, recv_sem, own_two, *sems
):
    me, mine = lax.axis_index("col"), lax.axis_index("row")
    rows = x_ref.shape[0] // PIECES
    greet_both(ncol, nrow, me, mine)
    relay, finish = line_gather(
        ncol,
        me,
        lambda c: x_ref.at[pl.ds(c * rows, rows)],
        lambda g, c: o_ref.at[g, pl.ds(c * rows, rows)],
        sems,
    )
    copies = []
    for k in range(1, nrow):
        peer = lax.rem(mine + k, nrow)
        copies.append(remote(g_ref, p_ref.at[mine], send_sem.at[k], recv_sem.at[k], "row", peer))
        copies[-1].start()
    own = pltpu.make_async_copy(x_ref, o_ref.at[me], own_sem)
    own.start()
    two = pltpu.make_async_copy(g_ref, p_ref.at[mine], own_two)
    two.start()
    own.wait()
    two.wait()
    relay()
    finish()
    for copy in copies:
        copy.wait()


def greet_both(ncol, nrow, me, mine):
    barrier = pltpu.get_barrier_semaphore()
    for k in range(1, ncol):
        pl.semaphore_signal(
            barrier, inc=1, device_id={"col": lax.rem(me + k, ncol)}, device_id_type=MESH
        )
    for k in range(1, nrow):
        pl.semaphore_signal(
            barrier, inc=1, device_id={"row": lax.rem(mine + k, nrow)}, device_id_type=MESH
        )
    pl.semaphore_wait(barrier, ncol + nrow - 2)


def add_into(out, rows, terms):
    def step(i, carry):
        at = pl.ds(pl.multiple_of(i * BAND, BAND), BAND)
        total = terms[0](at).astype(F32)
        for term in terms[1:]:
            total = total + term(at).astype(F32)
        out(at, total)
        return carry

    lax.fori_loop(0, rows // BAND, step, 0)


def col_sum_stages(
    n, me, x_ref, o_ref, x_buf, z_buf, stage, xs, xr, zs, zr, own_sem, *sems
):
    nz = n // 2
    z, x = me // 2, lax.rem(me, 2)
    other = me + 1 - 2 * x
    rows, width = x_ref.shape[0], x_ref.shape[1] // n
    part = rows // PIECES
    order = [lax.rem(z + k, nz) for k in (*range(1, nz), 0)]

    def first(to):
        src = columns(x_ref, to * 2 + 1 - x, width)
        return remote(src, x_buf.at[to], xs.at[to], xr.at[to], "col", other)

    def second(to):
        return remote(stage.at[to], z_buf.at[z], zs.at[to], zr.at[z], "col", to * 2 + x)

    def begin():
        for to in order:
            first(to).start()

    def pair(to):
        first(to).wait_recv()
        mine = pl.ds(pl.multiple_of((to * 2 + x) * width, width), width)

        def put(at, total):
            stage[to, at, :] = total.astype(BF)

        add_into(put, rows, [lambda at: x_ref[at, mine], lambda at: x_buf[to, at, :]])
        second(to).start()

    def view(g, c):
        return o_ref.at[
            pl.ds(c * part, part), pl.ds(pl.multiple_of(g * width, width), width)
        ]

    def gather():
        return line_gather(n, me, lambda c: stage.at[z, pl.ds(c * part, part)], view, sems)

    def total():
        first(z).wait_recv()
        for source in order[:-1]:
            block = z_buf.at[source]
            remote(block, block, zs.at[source], zr.at[source], "col", other).wait_recv()
        mine = pl.ds(pl.multiple_of(me * width, width), width)

        def put(at, value):
            stage[z, at, :] = value.astype(BF)

        terms = [lambda at: x_ref[at, mine], lambda at: x_buf[z, at, :]]
        for source in order[:-1]:
            terms.append(lambda at, source=source: z_buf[source, at, :])
        add_into(put, rows, terms)
        own = pltpu.make_async_copy(stage.at[z], columns(o_ref, me, width), own_sem)
        own.start()
        relay, finish = gather()
        own.wait()
        relay()
        finish()
        for to in order:
            first(to).wait_send()
        for to in order[:-1]:
            second(to).wait_send()

    return [begin, *[functools.partial(pair, to) for to in order[:-1]], total], first, pair


def col_sum_kernel(n, *refs):
    me = lax.axis_index("col")
    greet("col", n, me)
    for stage in col_sum_stages(n, me, *refs)[0]:
        stage()


def col_sum_scratch(n, rows, width):
    nz = n // 2
    sem = pltpu.SemaphoreType.DMA
    buf = pltpu.VMEM((nz, rows, width), BF)
    return [buf, buf, buf, *[sem((nz,))] * 4, sem, *gather_sems(n)]


def tile_sum(me, count, tile, part, o_ref, k_buf, y_buf, stage, ks, kr, ys, yr, gs, gr):
    y, k = me // 2, lax.rem(me, 2)
    other = me + 1 - 2 * k
    across = (1 - y) * 2 + k
    half = tile // 2
    mine = pl.ds(pl.multiple_of(k * half, half), half)
    theirs = pl.ds(pl.multiple_of((1 - k) * half, half), half)

    def spot(i):
        return pl.ds(pl.multiple_of(i * tile + k * half, half), half)

    def swap(i):
        return remote(part.at[i, :, theirs], k_buf.at[i], ks.at[i], kr.at[i], "row", other)

    def cross(i):
        return remote(stage.at[i], y_buf.at[i], ys.at[i], yr.at[i], "row", across)

    def hand(i):
        place = o_ref.at[:, spot(i)]
        return remote(place, place, gs.at[i], gr.at[i], "row", other)

    def middle(i):
        swap(i).wait_recv()
        stage[i] = (part[i, :, mine].astype(F32) + k_buf[i].astype(F32)).astype(BF)
        cross(i).start()

    def last(i):
        cross(i).wait_recv()
        o_ref[:, spot(i)] = (stage[i].astype(F32) + y_buf[i].astype(F32)).astype(BF)
        hand(i).start()

    def finish():
        def step(i, carry):
            swap(i).wait_send()
            cross(i).wait_send()
            hand(i).wait()
            return carry

        lax.fori_loop(0, count, step, 0)

    return swap, middle, last, finish


def tile_scratch(count, rows, tile):
    sem = pltpu.SemaphoreType.DMA
    half = pltpu.VMEM((count, rows, tile // 2), BF)
    return [pltpu.VMEM((count, rows, tile), BF), half, half, half, *[sem((count,))] * 6]


def tile_loop(count, compute, swap, middle, last, hooks):
    def step(i, carry):
        @pl.when(i < count)
        def _():
            compute(i)
            swap(i).start()

        @pl.when((i >= 1) & (i <= count))
        def _():
            middle(i - 1)

        @pl.when(i >= LAG)
        def _():
            last(i - LAG)

        for at, hook in hooks:
            pl.when(i == at)(hook)
        return carry

    lax.fori_loop(0, count + LAG, step, 0)


def stream_parts(n, me, a_ref, w_ref, o_ref, w_buf, w_sem, part, *rest):
    tile = w_buf.shape[2]
    count = w_ref.shape[1] // tile

    def fetch(i):
        at = pl.ds(pl.multiple_of(i * tile, tile), tile)
        slot = lax.rem(i, DEPTH)
        return pltpu.make_async_copy(w_ref.at[:, at], w_buf.at[slot], w_sem.at[slot])

    def compute(i):
        fetch(i).wait()

        @pl.when(i + DEPTH - 1 < count)
        def _():
            fetch(i + DEPTH - 1).start()

        product = jnp.dot(a_ref[...], w_buf[lax.rem(i, DEPTH)], preferred_element_type=F32)
        part[i] = product.astype(BF)

    for i in range(min(DEPTH - 1, count)):
        fetch(i).start()
    return count, compute, tile_sum(me, count, tile, part, o_ref, *rest)


def stream_scratch(count, rows, deep, tile):
    return [
        pltpu.VMEM((DEPTH, deep, tile), BF),
        pltpu.SemaphoreType.DMA((DEPTH,)),
        *tile_scratch(count, rows, tile),
    ]


def stream_kernel(n, a_ref, w_ref, o_ref, *scratch):
    me = lax.axis_index("row")
    count, compute, (swap, middle, last, finish) = stream_parts(
        n, me, a_ref, w_ref, o_ref, *scratch
    )
    greet("row", n, me)
    tile_loop(count, compute, swap, middle, last, [])
    finish()


def block_kernel(n, across, a_ref, w_ref, o_ref, w_buf, w_sem, part, *scratch):
    me = lax.axis_index("col")
    nz = n // 2
    z, x = me // 2, lax.rem(me, 2)
    width = o_ref.shape[1] // n

    def block(i):
        to = lax.rem(z + 1 + i // 2, nz)
        return to * 2 + x + (1 - 2 * x) * (1 - lax.rem(i, 2))

    def fetch(i):
        at = pl.ds(pl.multiple_of(block(i) * width, width), width)
        slot = lax.rem(i, DEPTH)
        src = w_ref.at[:, :, at] if across else w_ref.at[at]
        return pltpu.make_async_copy(src, w_buf.at[slot], w_sem.at[slot])

    for i in range(DEPTH - 1):
        fetch(i).start()
    stages, first, pair = col_sum_stages(n, me, part, o_ref, *scratch)
    greet("col", n, me)

    def step(i, carry):
        fetch(i).wait()

        @pl.when(i + DEPTH - 1 < n)
        def _():
            fetch(i + DEPTH - 1).start()

        slot = lax.rem(i, DEPTH)
        if across:
            pieces = [
                jnp.dot(a_ref[q], w_buf[slot, q], preferred_element_type=F32)
                for q in range(a_ref.shape[0])
            ]
            product = jnp.concatenate(pieces, axis=0)
        else:
            product = lax.dot_general(
                a_ref[...], w_buf[slot], (((1,), (1,)), ((), ())), preferred_element_type=F32
            )
        part[:, pl.ds(pl.multiple_of(block(i) * width, width), width)] = product.astype(BF)

        @pl.when(lax.rem(i, 2) == 0)
        def _():
            first(lax.rem(z + 1 + i // 2, nz)).start()

        @pl.when((lax.rem(i, 2) == 1) & (i >= 3))
        def _():
            pair(lax.rem(z + i // 2, nz))

        return carry

    lax.fori_loop(0, n, step, 0)
    stages[-1]()


def dot_col_sum(a, w, across, n, number):
    wide = w.shape[2] if across else w.shape[0]
    rows = a.shape[0] * a.shape[1] if across else a.shape[0]
    width = wide // n
    if not (fits(rows, width, n) and n >= 2 * DEPTH and wide % n == 0 and a.shape[-1] % 128 == 0):
        if across:
            product = jnp.einsum("qsj,qjp->qsp", a, w, preferred_element_type=F32)
        else:
            product = dot(a, w, ((1,), (1,)))
        return col_sum(product.astype(BF).reshape(rows, wide), n, number)
    shape = (*w.shape[:2], width) if across else (width, w.shape[1])
    scratch = [
        pltpu.VMEM((DEPTH, *shape), BF),
        pltpu.SemaphoreType.DMA((DEPTH,)),
        pltpu.VMEM((rows, wide), BF),
        *col_sum_scratch(n, rows, width),
    ]
    kernel = functools.partial(block_kernel, n, across)
    return launch(
        kernel, f"block{number}", number, (rows, wide), BF, scratch, a, w, specs=[VMEM, ANY]
    )


STREAM = 12


def stream_both_kernel(n, ncol, a_ref, w_ref, x_ref, o_ref, s_ref, *scratch):
    me, mine = lax.axis_index("row"), lax.axis_index("col")
    count, compute, (swap, middle, last, finish) = stream_parts(
        n, me, a_ref, w_ref, o_ref, *scratch[:STREAM]
    )
    greet_both(ncol, n, mine, me)
    begin, *pairs, total = col_sum_stages(ncol, mine, x_ref, s_ref, *scratch[STREAM:])[0]
    begin()
    hooks = [(GAP * (k + 1), pair) for k, pair in enumerate(pairs)]
    late = [pair for at, pair in hooks if at >= count + LAG]
    hooks = [hook for hook in hooks if hook[0] < count + LAG]
    tile_loop(count, compute, swap, middle, last, hooks)
    for pair in late:
        pair()
    total()
    finish()


def row_sum_kernel(
    n, pieces, x_ref, o_ref, k_buf, y_buf, stage, ks, kr, ys, yr, gs, gr
):
    me = lax.axis_index("row")
    ny = n // 2
    y, k = me // 2, lax.rem(me, 2)
    other = me + 1 - 2 * k
    width = x_ref.shape[1] // 2
    rows = x_ref.shape[0] // pieces
    mine = pl.ds(pl.multiple_of(k * width, width), width)
    theirs = pl.ds(pl.multiple_of((1 - k) * width, width), width)
    greet("row", n, me)
    parts = [pl.ds(c * rows, rows) for c in range(pieces)]
    swaps, sends, hands = [], {}, []
    for c, part in enumerate(parts):
        swaps.append(
            remote(x_ref.at[part, theirs], k_buf.at[part], ks.at[c], kr.at[c], "row", other)
        )
        swaps[-1].start()
    for c, part in enumerate(parts):
        swaps[c].wait_recv()

        def put(at, total, c=c):
            stage[pl.ds(pl.multiple_of(c * rows + at.start, BAND), BAND), :] = total.astype(BF)

        def shifted(at, c=c):
            return pl.ds(pl.multiple_of(c * rows + at.start, BAND), BAND)

        add_into(
            put,
            rows,
            [
                lambda at, s=shifted: x_ref[s(at), mine],
                lambda at, s=shifted: k_buf[s(at), :],
            ],
        )
        for d in range(1, ny):
            peer = lax.rem(y + d, ny) * 2 + k
            sends[c, d] = remote(
                stage.at[part], y_buf.at[d - 1, part], ys.at[d - 1, c], yr.at[d - 1, c], "row", peer
            )
            sends[c, d].start()
    for c, part in enumerate(parts):
        for d in range(1, ny):
            sends[c, d].wait_recv()

        def shifted(at, c=c):
            return pl.ds(pl.multiple_of(c * rows + at.start, BAND), BAND)

        def put(at, total, s=shifted):
            o_ref[s(at), mine] = total.astype(o_ref.dtype)

        terms = [lambda at, s=shifted: stage[s(at), :]]
        for d in range(1, ny):
            terms.append(lambda at, s=shifted, d=d: y_buf[d - 1, s(at), :])
        add_into(put, rows, terms)
        place = o_ref.at[part, mine]
        hands.append(remote(place, place, gs.at[c], gr.at[c], "row", other))
        hands[-1].start()
    for c in range(pieces):
        swaps[c].wait_send()
        for d in range(1, ny):
            sends[c, d].wait_send()
        hands[c].wait()


def launch(kernel, name, number, shape, dtype, scratch, *args, specs=None, outs=None, more=None):
    out = jax.ShapeDtypeStruct(shape, dtype)
    return pl.pallas_call(
        kernel,
        name=name,
        out_shape=out if more is None else [out, more],
        in_specs=specs or [VMEM] * len(args),
        out_specs=outs or (VMEM if more is None else [VMEM, VMEM]),
        scratch_shapes=scratch,
        compiler_params=pltpu.CompilerParams(
            collective_id=number, has_side_effects=True, vmem_limit_bytes=48 * 2**20
        ),
    )(*args)


def fits(rows, width, n, pieces=PIECES):
    return n % 2 == 0 and rows % (BAND * pieces) == 0 and width % 128 == 0


def gather_both(acts, grads, nrow, ncol, number):
    if not (fits(*acts.shape, ncol) and fits(*grads.shape, nrow)):
        full = lax.all_gather(acts, "col", axis=0, tiled=True)
        return full, lax.all_gather(grads, "row", axis=0, tiled=True)
    sem = pltpu.SemaphoreType.DMA
    scratch = [sem, sem((nrow,)), sem((nrow,)), sem, *gather_sems(ncol)]
    full, part = launch(
        functools.partial(gather_both_kernel, ncol, nrow),
        f"gather{number}",
        number,
        (ncol, *acts.shape),
        BF,
        scratch,
        acts,
        grads,
        more=jax.ShapeDtypeStruct((nrow, *grads.shape), BF),
    )
    return full.reshape(-1, acts.shape[1]), part.reshape(-1, grads.shape[1])


def streams(a, w, n):
    return n == 4 and a.shape[0] % BAND == 0 and a.shape[1] % 128 == 0 and w.shape[1] % TILE == 0


def dot_row_sum(a, w, n, number):
    if not streams(a, w, n):
        return row_sum(dot(a, w, ((1,), (0,))).astype(BF), n, number)
    rows, wide = a.shape[0], w.shape[1]
    scratch = stream_scratch(wide // TILE, rows, a.shape[1], TILE)
    kernel = functools.partial(stream_kernel, n)
    return launch(
        kernel, f"stream{number}", number, (rows, wide), BF, scratch, a, w, specs=[VMEM, ANY]
    )


def dot_both_sums(a, w, x, nrow, ncol, number):
    if not (streams(a, w, nrow) and fits(x.shape[0], x.shape[1] // ncol, ncol)):
        act = row_sum(dot(a, w, ((1,), (0,))).astype(BF), nrow, number)
        return act, col_sum(x, ncol, number + 20)
    rows, wide = a.shape[0], w.shape[1]
    scratch = [
        *stream_scratch(wide // TILE, rows, a.shape[1], TILE),
        *col_sum_scratch(ncol, x.shape[0], x.shape[1] // ncol),
    ]
    return launch(
        functools.partial(stream_both_kernel, nrow, ncol),
        f"stream{number}",
        number,
        (rows, wide),
        BF,
        scratch,
        a,
        w,
        x,
        specs=[VMEM, ANY, VMEM],
        more=jax.ShapeDtypeStruct(x.shape, BF),
    )


def col_sum(x, n, number):
    rows, width = x.shape[0], x.shape[1] // n
    if not fits(rows, width, n):
        return lax.psum(x.astype(F32), "col").astype(BF)
    scratch = col_sum_scratch(n, rows, width)
    kernel = functools.partial(col_sum_kernel, n)
    return launch(kernel, f"sum{number}", number, x.shape, BF, scratch, x)


def row_sum(x, n, number):
    rows, width = x.shape[0], x.shape[1] // 2
    if not fits(rows, width, n):
        return lax.psum(x.astype(F32), "row").astype(BF)
    ny = n // 2
    sem = pltpu.SemaphoreType.DMA
    scratch = [
        pltpu.VMEM((rows, width), BF),
        pltpu.VMEM((max(ny - 1, 1), rows, width), BF),
        pltpu.VMEM((rows, width), BF),
        sem((PIECES,)),
        sem((PIECES,)),
        sem((max(ny - 1, 1), PIECES)),
        sem((max(ny - 1, 1), PIECES)),
        sem((PIECES,)),
        sem((PIECES,)),
    ]
    kernel = functools.partial(row_sum_kernel, n, PIECES)
    return launch(kernel, f"sum{number}", number, x.shape, BF, scratch, x)


def factor_kernel(n, size, g_ref, o_ref, slots, work, send_sem, recv_sem):
    me = lax.axis_index("row")
    queries, high, wide = o_ref.shape
    greet("row", n, me)
    copies = []
    for k in range(1, n):
        peer = lax.rem(me + k, n)
        copies.append(
            remote(g_ref, slots.at[me], send_sem.at[k], recv_sem.at[k], "row", peer)
        )
        copies[-1].start()
    slots[me] = g_ref[...]
    for copy in copies:
        copy.wait()
    total = slots[0]
    for k in range(1, n):
        total = total + slots[k]
    work[...] = total
    row = lax.broadcasted_iota(jnp.int32, (high, wide), 0)
    lane = lax.broadcasted_iota(jnp.int32, (high, wide), 1)

    def step(k, carry):
        for q in range(queries):
            t = work[q]
            top = work[q, pl.ds(k, 1), :]
            column = jnp.sum(jnp.where(lane == k, t, 0.0), axis=1, keepdims=True)
            pivot = jnp.sum(jnp.where(lane[:1] == k, top, 0.0), axis=1, keepdims=True)
            part = column / pivot
            top = jnp.where(lane[:1] == k, 0.0, top)
            base = jnp.where(lane == k, 0.0, t)
            moved = jnp.where(lane == k, -part, base - part * top)
            work[q] = jnp.where(row > k, moved, t)
        return carry

    lax.fori_loop(0, size, step, 0)
    for q in range(queries):
        t = work[q]
        diagonal = jnp.sum(jnp.where(lane == row, t, 0.0), axis=1, keepdims=True)
        scale = lax.rsqrt(diagonal)
        scale = scale * (1.5 - 0.5 * diagonal * scale * scale)
        o_ref[q] = jnp.where(lane < row, t * scale, jnp.where(lane == row, scale, 0.0))


def inverse_factor(gram, n, number):
    queries, size, _ = gram.shape
    if n % 2 or size > 128 or size % 8:
        factor = jnp.linalg.cholesky(lax.psum(gram, "row"))
        unit = jnp.broadcast_to(jnp.eye(size, dtype=F32), gram.shape)
        return lax.linalg.triangular_solve(factor, unit, left_side=True, lower=True)
    wide = jnp.pad(gram, ((0, 0), (0, 0), (0, 128 - size)))
    sem = pltpu.SemaphoreType.DMA
    scratch = [pltpu.VMEM((n, *wide.shape), F32), pltpu.VMEM(wide.shape, F32), sem((n,)), sem((n,))]
    kernel = functools.partial(factor_kernel, n, size)
    return launch(kernel, f"factor{number}", number, wide.shape, F32, scratch, wide)[:, :, :size]


def query_rows(value, q, queries, blocks):
    rows, wide = value.shape
    split = value.astype(F32).reshape(blocks, queries, rows // (blocks * queries), wide)
    return split[:, q].reshape(rows // queries, wide).astype(BF)


def scale_kernel(
    n, blocks, queries, act_ref, grad_ref, sketch_ref, eigen_ref, scaled_ref, o_ref,
    grad_buf, e_buf, s_buf, e_sem, s_sem, part, *rest,
):
    me = lax.axis_index("row")
    tile = e_buf.shape[1]
    count = eigen_ref.shape[0] // tile
    size = sketch_ref.shape[0]
    swap, middle, last, finish = tile_sum(me, count, tile, part, o_ref, *rest)

    def fetch(i):
        at = pl.ds(pl.multiple_of(i * tile, tile), tile)
        slot = lax.rem(i, DEPTH)
        return pltpu.make_async_copy(eigen_ref.at[at], e_buf.at[slot], e_sem.at[slot])

    def store(i):
        at = pl.ds(pl.multiple_of(i * tile, tile), tile)
        slot = lax.rem(i, 2)
        return pltpu.make_async_copy(s_buf.at[slot], scaled_ref.at[:, at], s_sem.at[slot])

    for i in range(min(DEPTH - 1, count)):
        fetch(i).start()
    for q in range(queries):
        for c in range(grad_ref.shape[1] // tile):
            at = pl.ds(c * tile, tile)
            grad_buf[q, :, at] = query_rows(grad_ref[:, at], q, queries, blocks[1])
    greet("row", n, me)

    def compute(i):
        fetch(i).wait()

        @pl.when(i + DEPTH - 1 < count)
        def _():
            fetch(i + DEPTH - 1).start()

        @pl.when(i >= 2)
        def _():
            store(i - 2).wait()

        slot = lax.rem(i, 2)
        inverse = 1.0 / e_buf[lax.rem(i, DEPTH)].astype(F32)
        act = act_ref[:, pl.ds(pl.multiple_of(i * tile, tile), tile)]
        pieces = []
        for q in range(queries):
            total = lax.dot_general(
                query_rows(act, q, queries, blocks[0]),
                grad_buf[q],
                (((0,), (0,)), ((), ())),
                preferred_element_type=F32,
            )
            scaled = (total * inverse).astype(BF)
            s_buf[slot, q] = scaled
            pieces.append(
                lax.dot_general(
                    sketch_ref[...], scaled, (((1,), (1,)), ((), ())), preferred_element_type=F32
                )
            )
        part[i] = jnp.concatenate(pieces, axis=0).astype(BF)
        store(i).start()

    tile_loop(count, compute, swap, middle, last, [])
    finish()
    for i in range(max(count - 2, 0), count):
        store(i).wait()


def scale_and_reduce(act, grad, eigen, sketch, queries, blocks, n, number):
    rows, wide = act.shape
    deep = grad.shape[1]
    size = sketch.shape[0]
    ok = n == 4 and wide % TILE == 0 and deep % TILE == 0 and size % 8 == 0
    ok = ok and queries * size % BAND == 0 and rows // queries % BAND == 0
    if not (ok and all(rows % (8 * queries * b) == 0 for b in blocks)):
        act = act.reshape(blocks[0], queries, -1, wide)
        grad = grad.reshape(blocks[1], queries, -1, deep)
        act = act.transpose(1, 0, 2, 3).reshape(queries, -1, wide)
        grad = grad.transpose(1, 0, 2, 3).reshape(queries, -1, deep)
        total = jnp.einsum("qtj,qtp->qjp", act, grad, preferred_element_type=F32)
        scaled = (total / eigen.astype(F32)).astype(BF)
        part = jnp.einsum("qjp,sp->qsj", scaled, sketch, preferred_element_type=F32)
        return scaled, row_sum(part.astype(BF).reshape(queries * size, wide), n, number)
    sem = pltpu.SemaphoreType.DMA
    scratch = [
        pltpu.VMEM((queries, rows // queries, deep), BF),
        pltpu.VMEM((DEPTH, TILE, deep), BF),
        pltpu.VMEM((2, queries, TILE, deep), BF),
        sem((DEPTH,)),
        sem((2,)),
        *tile_scratch(wide // TILE, queries * size, TILE),
    ]
    return launch(
        functools.partial(scale_kernel, n, blocks, queries),
        f"scale{number}",
        number,
        (queries, wide, deep),
        BF,
        scratch,
        act,
        grad,
        sketch,
        eigen,
        specs=[VMEM, VMEM, VMEM, ANY],
        outs=[ANY, VMEM],
        more=jax.ShapeDtypeStruct((queries * size, wide), BF),
    )


def dot(a, b, contract):
    return lax.dot_general(a, b, ((contract), ((), ())), preferred_element_type=F32)


def on_device(nrow, ncol, acts, grads, basis_in, basis_out, eigen, sketch):
    queries = acts.shape[1]
    size = sketch.shape[0]
    flat = queries * size
    full_acts, full_grads = gather_both(
        acts.transpose(1, 0, 2).reshape(-1, acts.shape[2]),
        grads.transpose(1, 0, 2).reshape(-1, grads.shape[2]),
        nrow,
        ncol,
        0,
    )
    rows = full_grads.shape[0]
    joined = jnp.concatenate([full_grads, sketch], axis=0)
    joined = jnp.pad(joined, ((0, -joined.shape[0] % (BAND * PIECES)), (0, 0)))
    joined_part = dot(joined, basis_out, ((1,), (0,))).astype(BF)
    act_rot, joined_sum = dot_both_sums(full_acts, basis_in, joined_part, nrow, ncol, 1)
    grad_rot, sketch_rot = joined_sum[:rows], joined_sum[rows : rows + size]
    scaled, reduced = scale_and_reduce(
        act_rot, grad_rot, eigen, sketch_rot, queries, (ncol, nrow), nrow, 2
    )
    range_rows = dot_col_sum(reduced, basis_in, False, ncol, 5).reshape(queries, size, -1)
    gram = jnp.einsum("qsi,qri->qsr", range_rows, range_rows, preferred_element_type=F32)
    inverse = inverse_factor(gram, nrow, 6)
    range_basis = jnp.einsum(
        "qsr,qri->qsi", inverse, range_rows.astype(F32), precision=lax.Precision.HIGHEST
    )
    basis_rows = range_basis.astype(BF).reshape(flat, -1)
    mapped = dot_row_sum(basis_rows, basis_in, nrow, 7)
    mapped = mapped.reshape(queries, size, -1)
    core = dot_col_sum(mapped, scaled, True, ncol, 8)
    projection_part = dot(core, basis_out, ((1,), (1,))).astype(BF)
    projected = row_sum(projection_part, nrow, 9)
    return range_basis, projected.astype(F32).reshape(queries, size, -1)


def solution(mesh):
    in_specs = (
        P("col", None, "row"),
        P("row", None, "col"),
        P("row", "col"),
        P("col", "row"),
        P("col", "row"),
        P(None, "col"),
    )
    out_specs = (P(None, None, "row"), P(None, None, "col"))
    body = functools.partial(on_device, mesh.shape["row"], mesh.shape["col"])
    return jax.shard_map(body, mesh=mesh, in_specs=in_specs, out_specs=out_specs, check_vma=False)
```
